32 devices in a mesh: data: 2 (over x), cp: 16 (over z, y, core).
Axes of the slice: x: 2, y: 2, z: 4, core: 2. Of those that a mesh axis runs over, the one named last changes fastest.
Arguments:
- q: bfloat16 [16384, 8, 128], P(('data', 'cp')), parts along dimension 0
- k: bfloat16 [16384, 8, 128], P(('data', 'cp')), parts along dimension 0
- v: bfloat16 [16384, 8, 128], P(('data', 'cp')), parts along dimension 0
- o: bfloat16 [16384, 8, 128], P(('data', 'cp')), parts along dimension 0
- dout: bfloat16 [16384, 8, 128], P(('data', 'cp')), parts along dimension 0
- lse: float32 [8, 16384], P(None, ('data', 'cp')), parts along dimension 1
Outputs:
- output 1: bfloat16 [16384, 8, 128], P(('data', 'cp')), parts along dimension 0
- output 2: bfloat16 [16384, 8, 128], P(('data', 'cp')), parts along dimension 0
- output 3: bfloat16 [16384, 8, 128], P(('data', 'cp')), parts along dimension 0
There are 2 independent parts. The reference program is written for one: setup_inputs(seed, part) draws one part's arguments, and reference() takes and returns one part's arrays. A program takes and returns all parts, laid end to end along the dimension named above; each array names one.
All inputs are finite; a program needn't handle non-finite values.
Results may differ from the reference program's by a relative error of at most 0.001.
Values are sent between devices in bfloat16 or wider.
A program may use at most 1 GiB of HBM per device.

```python
import math
import jax
import jax.numpy as jnp
from jax import lax

C = 512
CP = 16
HEADS = 8
HEAD = 128
QB = 128

T = C * CP
SCALE = 1.0 / math.sqrt(HEAD)


def positions():
    r = jnp.arange(T, dtype=jnp.int32)
    return (r % C) * CP + r // C


def _head_forward(q, k, v, pos):
    def blk(b):
        qb = lax.dynamic_slice_in_dim(q, b * QB, QB)
        pb = lax.dynamic_slice_in_dim(pos, b * QB, QB)
        s = jnp.dot(qb, k.T, preferred_element_type=jnp.float32) * SCALE
        s = jnp.where(pos[None, :] <= pb[:, None], s, -jnp.inf)
        mx = jnp.max(s, axis=1, keepdims=True)
        e = jnp.exp(s - mx)
        l = jnp.sum(e, axis=1, keepdims=True)
        o = jnp.dot((e / l).astype(jnp.bfloat16), v, preferred_element_type=jnp.float32)
        return o.astype(jnp.bfloat16), (mx + jnp.log(l))[:, 0]
    o, lse = lax.map(blk, jnp.arange(T // QB))
    return o.reshape(T, HEAD), lse.reshape(T)


def _forward(q, k, v):
    pos = positions()
    o, lse = lax.map(lambda a: _head_forward(a[0], a[1], a[2], pos),
                     (q.transpose(1, 0, 2), k.transpose(1, 0, 2), v.transpose(1, 0, 2)))
    return o.transpose(1, 0, 2), lse


def setup_inputs(seed: int = 0, part: int = 0) -> dict:
    key = jax.random.fold_in(jax.random.PRNGKey(seed), part)
    kq, kk, km, kv, kd = jax.random.split(key, 5)
    shape = (T, HEADS, HEAD)
    q = jax.random.normal(kq, shape, jnp.float32).astype(jnp.bfloat16)
    k = jax.random.normal(kk, shape, jnp.float32).astype(jnp.bfloat16)
    mu = jax.random.normal(km, (1, HEADS, HEAD), jnp.float32)
    v = (0.8 * mu + 0.6 * jax.random.normal(kv, shape, jnp.float32)).astype(jnp.bfloat16)
    o, lse = _forward(q, k, v)
    dout = (0.8 * o.astype(jnp.float32) + 0.6 * jax.random.normal(kd, shape, jnp.float32)).astype(jnp.bfloat16)
    return {'q': q, 'k': k, 'v': v, 'o': o, 'dout': dout, 'lse': lse}


def reference(q, k, v, o, dout, lse):
    pos = positions()
    dd = jnp.sum(dout.astype(jnp.float32) * o.astype(jnp.float32), axis=-1)

    def head(a):
        qh, kh, vh, doh, lh, dh = a

        def step(carry, b):
            dk, dv = carry
            qb = lax.dynamic_slice_in_dim(qh, b * QB, QB)
            dob = lax.dynamic_slice_in_dim(doh, b * QB, QB)
            lb = lax.dynamic_slice_in_dim(lh, b * QB, QB)
            db = lax.dynamic_slice_in_dim(dh, b * QB, QB)
            pb = lax.dynamic_slice_in_dim(pos, b * QB, QB)
            s = jnp.dot(qb, kh.T, preferred_element_type=jnp.float32) * SCALE
            mask = pos[None, :] <= pb[:, None]
            p = jnp.where(mask, jnp.exp(s - lb[:, None]), 0.0)
            dv = dv + jnp.dot(p.astype(jnp.bfloat16).T, dob, preferred_element_type=jnp.float32)
            dp = jnp.dot(dob, vh.T, preferred_element_type=jnp.float32)
            ds = (p * (dp - db[:, None])).astype(jnp.bfloat16)
            dqb = jnp.dot(ds, kh, preferred_element_type=jnp.float32) * SCALE
            dk = dk + jnp.dot(ds.T, qb, preferred_element_type=jnp.float32) * SCALE
            return (dk, dv), dqb

        z = jnp.zeros((T, HEAD), jnp.float32)
        (dk, dv), dq = lax.scan(step, (z, z), jnp.arange(T // QB))
        return dq.reshape(T, HEAD), dk, dv

    dq, dk, dv = lax.map(head, (q.transpose(1, 0, 2), k.transpose(1, 0, 2), v.transpose(1, 0, 2),
                                dout.transpose(1, 0, 2), lse, dd.T))
    return (dq.transpose(1, 0, 2).astype(jnp.bfloat16),
            dk.transpose(1, 0, 2).astype(jnp.bfloat16),
            dv.transpose(1, 0, 2).astype(jnp.bfloat16))
```

```python
import functools
import math

import jax
import jax.numpy as jnp
from jax import lax
from jax.experimental import pallas as pl
from jax.experimental.pallas import tpu as pltpu
from jax.sharding import PartitionSpec as P

MESH = pl.DeviceIdType.MESH
F32 = jnp.float32
BF16 = jnp.bfloat16

CH = 8
R = 32
C = 16
KB = CH * R
QB = 2 * KB
D = 128
NT = (((1,), (1,)), ((), ()))
TN = (((0,), (0,)), ((), ()))
LOG2E = math.log2(math.e)
SCALE = D ** -0.5


def _kernel(q_ref, k_ref, v_ref, do_ref, stat_ref, dq_out, dk_out, dv_out,
            stage, buf, statbuf, rows, dq, dqin, dqs, kvs, rkv, rq, tmp, dk_acc, dv_acc,
            s_in, r_in, s_fw, r_fw, s_kv, r_kv, s_x, r_x, s_q, r_q, s_st, r_st):
    cp = lax.axis_index('cp')
    chip = cp // 2
    core = cp % 2
    sib = {'cp': chip * 2 + 1 - core}

    def peer(i):
        return lax.rem(chip + i, CH)

    def dev(h):
        return {'cp': h * 2 + core}

    def rcopy(src, dst, ss, rs, to):
        return pltpu.make_async_remote_copy(src_ref=src, dst_ref=dst, send_sem=ss, recv_sem=rs,
                                            device_id=to, device_id_type=MESH)

    barrier = pltpu.get_barrier_semaphore()
    pl.semaphore_signal(barrier, inc=1, device_id=sib, device_id_type=MESH)
    for i in range(1, CH):
        pl.semaphore_signal(barrier, inc=1, device_id=dev(peer(i)), device_id_type=MESH)
    pl.semaphore_wait(barrier, CH)

    statbuf[core, chip] = stat_ref[chip]
    for i in range(1, CH):
        h = peer(i)
        rcopy(stat_ref.at[h], statbuf.at[core, chip], s_st.at[0], r_st.at[0], dev(h)).start()

    def gather(c):
        for t, ref in enumerate((k_ref, v_ref, q_ref, do_ref)):
            tmp[t] = ref[pl.ds(pl.multiple_of(c * KB, KB), KB), :].astype(F32)
            for h in range(CH):
                stage[c, h, t] = tmp[t, pl.ds(h, R, stride=CH), :].astype(BF16)
        buf[c, core, chip] = stage[c, chip]

    def send(c):
        for i in range(1, CH):
            h = peer(i)
            rcopy(stage.at[c, h], buf.at[c, core, chip], s_in.at[c], r_in.at[c], dev(h)).start()

    gather(C - 1)

    def prologue(n, _):
        c = C - 1 - n

        @pl.when(c > 0)
        def _():
            gather(c - 1)
        send(c)
        return 0

    lax.fori_loop(0, C, prologue, 0)

    rcopy(statbuf.at[core, pl.ds(0, CH - 1)], statbuf.at[core, pl.ds(0, CH - 1)],
          s_st.at[0], r_st.at[0], sib).wait_recv()
    fst = rcopy(statbuf.at[core], statbuf.at[core], s_st.at[1], r_st.at[1], sib)
    fst.start()
    rcopy(statbuf.at[1 - core], statbuf.at[1 - core], s_st.at[1], r_st.at[1], sib).wait_recv()
    quarter = lax.broadcasted_iota(jnp.int32, (1, 128), 1) // R
    for st in range(2):
        mul = LOG2E if st == 0 else 1.0
        for t in range(4):
            for g in range(4):
                src = [statbuf[g // 2, (g % 2) * 4 + m, :, st * 512 + t * 128:st * 512 + t * 128 + 128] * mul
                       for m in range(4)]
                for r in range(4):
                    acc = jnp.zeros((1, 128), F32)
                    for m in range(4):
                        sh = ((m - r) % 4) * R
                        x = pltpu.roll(src[m], sh, 1) if sh else src[m]
                        acc = jnp.where(quarter == m, x, acc)
                    rows[4 * t + r, st:st + 1, g * 128:(g + 1) * 128] = acc

    def diag_mask():
        ki = lax.broadcasted_iota(jnp.int32, (KB, QB), 0)
        qi = lax.broadcasted_iota(jnp.int32, (KB, QB), 1)
        kpos = (ki % R) * 16 + (ki // R) * 2 + core
        qpos = (qi % R) * 16 + ((qi // R) % CH) * 2 + qi // KB
        return kpos <= qpos

    def tile(c, b, diag):
        kk = buf[c, core, :, 0].reshape(KB, D)
        vv = buf[c, core, :, 1].reshape(KB, D)
        qq = buf[b, :, :, 2].reshape(QB, D)
        dd = buf[b, :, :, 3].reshape(QB, D)
        s = lax.dot_general(kk, qq, NT, preferred_element_type=F32)
        p = jnp.exp2(s * (SCALE * LOG2E) - rows[b, 0:1, :])
        if diag:
            p = jnp.where(diag_mask(), p, 0.0)
        dp = lax.dot_general(vv, dd, NT, preferred_element_type=F32)
        dv = jnp.dot(p.astype(BF16), dd, preferred_element_type=F32)
        ds = (p * (dp - rows[b, 1:2, :])).astype(BF16)
        dk = jnp.dot(ds, qq, preferred_element_type=F32)
        dqb = lax.dot_general(ds, kk, TN, preferred_element_type=F32)
        if diag:
            dv_acc[...] = dv
            dk_acc[...] = dk
            dq[b] = dqb.reshape(2, KB, D)
        else:
            dv_acc[...] += dv
            dk_acc[...] += dk
            dq[b] += dqb.reshape(2, KB, D)

    def arrive(c):
        rcopy(buf.at[c, core, pl.ds(0, CH - 1)], buf.at[c, core, pl.ds(0, CH - 1)],
              s_in.at[c], r_in.at[c], sib).wait_recv()
        rcopy(buf.at[c, core, :, pl.ds(2, 2)], buf.at[c, core, :, pl.ds(2, 2)],
              s_fw.at[c], r_fw.at[c], sib).start()

    def forwarded(c):
        return rcopy(buf.at[c, 1 - core, :, pl.ds(2, 2)], buf.at[c, 1 - core, :, pl.ds(2, 2)],
                     s_fw.at[c], r_fw.at[c], sib)

    def give_kv(c):
        kvs[c, :, 0] = (dk_acc[...] * SCALE).astype(BF16).reshape(CH, R, D)
        kvs[c, :, 1] = dv_acc[...].astype(BF16).reshape(CH, R, D)
        rkv[c, chip] = kvs[c, chip]
        for i in range(1, CH):
            h = peer(i)
            rcopy(kvs.at[c, h], rkv.at[c, chip], s_kv.at[c], r_kv.at[c], dev(h)).start()

    def step(n, _):
        c = C - 1 - n
        arrive(c)
        forwarded(c).wait_recv()
        tile(c, c, True)
        lax.fori_loop(c + 1, C, lambda b, _: (tile(c, b, False), 0)[1], 0)
        give_kv(c)
        return 0

    lax.fori_loop(0, C - 1, step, 0)

    def swap(b):
        rcopy(dq.at[b, 1 - core], dqin.at[b], s_x.at[b], r_x.at[b], sib).start()

    def give_q(b):
        rcopy(dq.at[b, core], dqin.at[b], s_x.at[b], r_x.at[b], sib).wait_recv()
        dqs[b] = ((dq[b, core] + dqin[b]) * SCALE).astype(BF16).reshape(CH, R, D)
        rq[b, chip] = dqs[b, chip]
        for i in range(1, CH):
            h = peer(i)
            rcopy(dqs.at[b, h], rq.at[b, chip], s_q.at[b], r_q.at[b], dev(h)).start()

    arrive(0)
    forwarded(0).wait_recv()
    tile(0, 0, True)
    swap(0)

    def last(b, _):
        tile(0, b, False)
        swap(b)
        give_q(b - 1)
        return 0

    lax.fori_loop(1, C, last, 0)
    give_kv(0)
    give_q(C - 1)

    def put_kv(n, _):
        c = C - 1 - n
        rcopy(kvs.at[c, pl.ds(0, CH - 1)], rkv.at[c, pl.ds(0, CH - 1)], s_kv.at[c], r_kv.at[c], sib).wait_recv()
        for t, ref in enumerate((dk_out, dv_out)):
            for h in range(CH):
                tmp[t, pl.ds(h, R, stride=CH), :] = rkv[c, h, t].astype(F32)
            ref[pl.ds(pl.multiple_of(c * KB, KB), KB), :] = tmp[t].astype(BF16)
        return 0

    lax.fori_loop(0, C, put_kv, 0)

    def put_q(c, _):
        rcopy(dqs.at[c, pl.ds(0, CH - 1)], rq.at[c, pl.ds(0, CH - 1)], s_q.at[c], r_q.at[c], sib).wait_recv()
        for h in range(CH):
            tmp[2, pl.ds(h, R, stride=CH), :] = rq[c, h].astype(F32)
        dq_out[pl.ds(pl.multiple_of(c * KB, KB), KB), :] = tmp[2].astype(BF16)
        return 0

    lax.fori_loop(0, C, put_q, 0)

    rcopy(statbuf.at[core, pl.ds(0, CH - 1)], statbuf.at[core, pl.ds(0, CH - 1)],
          s_st.at[0], r_st.at[0], sib).wait_send()
    fst.wait_send()

    def drain(c, _):
        rcopy(stage.at[c, pl.ds(0, CH - 1)], buf.at[c, core, pl.ds(0, CH - 1)], s_in.at[c], r_in.at[c], sib).wait_send()
        forwarded(c).wait_send()
        rcopy(kvs.at[c, pl.ds(0, CH - 1)], rkv.at[c, pl.ds(0, CH - 1)], s_kv.at[c], r_kv.at[c], sib).wait_send()
        rcopy(dq.at[c, core], dqin.at[c], s_x.at[c], r_x.at[c], sib).wait_send()
        rcopy(dqs.at[c, pl.ds(0, CH - 1)], rq.at[c, pl.ds(0, CH - 1)], s_q.at[c], r_q.at[c], sib).wait_send()
        return 0

    lax.fori_loop(0, C, drain, 0)


def solution(mesh):
    rows = P(('data', 'cp'))
    cols = P(None, ('data', 'cp'))

    def local(q, k, v, o, dout, lse):
        c, h, d = q.shape
        dd = jnp.einsum('qhd,qhd->hq', dout, o, preferred_element_type=F32)
        stat = jnp.concatenate([lse, dd], axis=1).reshape(h, 1, 2 * c)
        flat = lambda x: x.reshape(c * h, d)
        vm = pl.BlockSpec(memory_space=pltpu.VMEM)
        sem = pltpu.SemaphoreType.DMA
        outs = pl.pallas_call(
            _kernel,
            out_shape=[jax.ShapeDtypeStruct((c * h, d), BF16)] * 3,
            in_specs=[vm] * 5,
            out_specs=[vm] * 3,
            scratch_shapes=[
                pltpu.VMEM((C, CH, 4, R, D), BF16),
                pltpu.VMEM((C, 2, CH, 4, R, D), BF16),
                pltpu.VMEM((2, CH, 1, 2 * c), F32),
                pltpu.VMEM((C, 8, QB), F32),
                pltpu.VMEM((C, 2, KB, D), F32),
                pltpu.VMEM((C, KB, D), F32),
                pltpu.VMEM((C, CH, R, D), BF16),
                pltpu.VMEM((C, CH, 2, R, D), BF16),
                pltpu.VMEM((C, CH, 2, R, D), BF16),
                pltpu.VMEM((C, CH, R, D), BF16),
                pltpu.VMEM((4, KB, D), F32),
                pltpu.VMEM((KB, D), F32),
                pltpu.VMEM((KB, D), F32),
            ] + [sem((C,))] * 10 + [sem((2,))] * 2,
            compiler_params=pltpu.CompilerParams(collective_id=0, has_side_effects=True,
                                                 vmem_limit_bytes=60 * 2 ** 20),
        )(flat(q), flat(k), flat(v), flat(dout), stat)
        return tuple(x.reshape(c, h, d) for x in outs)

    return jax.shard_map(local, mesh=mesh, in_specs=(rows, rows, rows, rows, rows, cols),
                         out_specs=(rows, rows, rows), check_vma=False)
```

```python
import functools
import math

import jax
import jax.numpy as jnp
from jax import lax
from jax.experimental import pallas as pl
from jax.experimental.pallas import tpu as pltpu
from jax.sharding import PartitionSpec as P

MESH = pl.DeviceIdType.MESH
F32 = jnp.float32
BF16 = jnp.bfloat16

CH = 8
R = 32
C = 16
KB = CH * R
QB = 2 * KB
D = 128
NT = (((1,), (1,)), ((), ()))
TN = (((0,), (0,)), ((), ()))
LOG2E = math.log2(math.e)
U = 4
SCALE = D ** -0.5


def _kernel(k_hbm, v_hbm, q_hbm, do_hbm, o_hbm, lse_hbm, dq_out, dk_out, dv_out,
            xin, lsev, stage, ostage, statloc, buf, statbuf, rows, dq, dqin, dqs, kvs, rkv, rq, tmp, dk_acc, dv_acc,
            s_in, r_in, s_fw, r_fw, s_kv, r_kv, s_x, r_x, s_q, r_q, s_st, r_st, s_ld):
    cp = lax.axis_index('cp')
    chip = cp // 2
    core = cp % 2
    sib = {'cp': chip * 2 + 1 - core}

    hbm = (k_hbm, v_hbm, q_hbm, do_hbm, o_hbm)
    lead = (C - 1) * KB
    loads = []
    for t in range(4):
        loads.append(pltpu.make_async_copy(hbm[t].at[pl.ds(lead, KB)], xin.at[t, pl.ds(lead, KB)], s_ld.at[0, t]))
    for t in range(4):
        loads.append(pltpu.make_async_copy(hbm[t].at[pl.ds(0, lead)], xin.at[t, pl.ds(0, lead)], s_ld.at[1, t]))
    loads.append(pltpu.make_async_copy(o_hbm, xin.at[4], s_ld.at[0, 4]))
    loads.append(pltpu.make_async_copy(lse_hbm, lsev, s_ld.at[1, 4]))
    for x in loads:
        x.start()

    def peer(i):
        return lax.rem(chip + i, CH)

    def dev(h):
        return {'cp': h * 2 + core}

    def rcopy(src, dst, ss, rs, to):
        return pltpu.make_async_remote_copy(src_ref=src, dst_ref=dst, send_sem=ss, recv_sem=rs,
                                            device_id=to, device_id_type=MESH)

    def gather(c):
        r0 = pl.multiple_of(c * KB, KB)
        for t in range(4):
            tmp[t] = xin[t, pl.ds(r0, KB), :].astype(F32)
            for h in range(CH):
                stage[c, h, t] = tmp[t, pl.ds(h, R, stride=CH), :].astype(BF16)
        buf[c, core, chip] = stage[c, chip]

    def gather_o(c):
        tmp[4] = xin[4, pl.ds(pl.multiple_of(c * KB, KB), KB), :].astype(F32)
        for h in range(CH):
            ostage[c, h] = tmp[4, pl.ds(h, R, stride=CH), :].astype(BF16)

    def send(c):
        for i in range(1, CH):
            h = peer(i)
            rcopy(stage.at[c, h], buf.at[c, core, chip], s_in.at[c], r_in.at[c], dev(h)).start()

    def loop(lo, hi, f):
        lax.fori_loop(lo, hi, lambda x, _: (f(x), 0)[1], 0)

    barrier = pltpu.get_barrier_semaphore()
    pl.semaphore_signal(barrier, inc=1, device_id=sib, device_id_type=MESH)
    for i in range(1, CH):
        pl.semaphore_signal(barrier, inc=1, device_id=dev(peer(i)), device_id_type=MESH)
    for x in loads[:4]:
        x.wait()
    gather(C - 1)
    pl.semaphore_wait(barrier, CH)
    send(C - 1)
    for x in loads[4:]:
        x.wait()
    gather(C - 2)
    gather(C - 3)
    send(C - 2)
    gather(C - 4)
    send(C - 3)
    loop(0, C - 4, lambda n: gather(C - 5 - n))
    send(C - 4)
    loop(0, C, gather_o)

    ones = jnp.ones((8, D), BF16)
    for h in range(CH):
        x = (stage[:, h, 3].astype(F32) * ostage[:, h].astype(F32)).reshape(C * R, D)
        hi = x.astype(BF16)
        lo = (x - hi.astype(F32)).astype(BF16)
        e = (lax.dot_general(ones, hi, NT, preferred_element_type=F32)
             + lax.dot_general(ones, lo, NT, preferred_element_type=F32))
        statloc[h, :, :C * R] = lsev[h:h + 1, :]
        statloc[h, :, C * R:] = e[0:1, :]
    statbuf[core, chip] = statloc[chip]
    for i in range(1, CH):
        h = peer(i)
        rcopy(statloc.at[h], statbuf.at[core, chip], s_st.at[0], r_st.at[0], dev(h)).start()
    loop(0, C - 4, lambda n: send(C - 5 - n))

    def arrive(c):
        rcopy(buf.at[c, core, pl.ds(0, CH - 1)], buf.at[c, core, pl.ds(0, CH - 1)],
              s_in.at[c], r_in.at[c], sib).wait_recv()
        rcopy(buf.at[c, core, :, pl.ds(2, 2)], buf.at[c, core, :, pl.ds(2, 2)],
              s_fw.at[c], r_fw.at[c], sib).start()

    def forwarded(c):
        return rcopy(buf.at[c, 1 - core, :, pl.ds(2, 2)], buf.at[c, 1 - core, :, pl.ds(2, 2)],
                     s_fw.at[c], r_fw.at[c], sib)

    arrive(C - 1)
    rcopy(statbuf.at[core, pl.ds(0, CH - 1)], statbuf.at[core, pl.ds(0, CH - 1)],
          s_st.at[0], r_st.at[0], sib).wait_recv()
    fst = rcopy(statbuf.at[core], statbuf.at[core], s_st.at[1], r_st.at[1], sib)
    fst.start()
    rcopy(statbuf.at[1 - core], statbuf.at[1 - core], s_st.at[1], r_st.at[1], sib).wait_recv()
    quarter = lax.broadcasted_iota(jnp.int32, (1, 128), 1) // R
    for st in range(2):
        mul = LOG2E if st == 0 else 1.0
        for t in range(4):
            for g in range(4):
                src = [statbuf[g // 2, (g % 2) * 4 + m, :, st * 512 + t * 128:st * 512 + t * 128 + 128] * mul
                       for m in range(4)]
                for r in range(4):
                    acc = jnp.zeros((1, 128), F32)
                    for m in range(4):
                        sh = ((m - r) % 4) * R
                        x = pltpu.roll(src[m], sh, 1) if sh else src[m]
                        acc = jnp.where(quarter == m, x, acc)
                    rows[4 * t + r, st:st + 1, g * 128:(g + 1) * 128] = acc

    def diag_mask():
        ki = lax.broadcasted_iota(jnp.int32, (KB, QB), 0)
        qi = lax.broadcasted_iota(jnp.int32, (KB, QB), 1)
        kpos = (ki % R) * 16 + (ki // R) * 2 + core
        qpos = (qi % R) * 16 + ((qi // R) % CH) * 2 + qi // KB
        return kpos <= qpos

    def clear():
        dk_acc[...] = jnp.zeros_like(dk_acc)
        dv_acc[...] = jnp.zeros_like(dv_acc)

    def tile(c, b, diag):
        kk = buf[c, core, :, 0].reshape(KB, D)
        vv = buf[c, core, :, 1].reshape(KB, D)
        qq = buf[b, :, :, 2].reshape(QB, D)
        dd = buf[b, :, :, 3].reshape(QB, D)
        s = lax.dot_general(kk, qq, NT, preferred_element_type=F32)
        p = jnp.exp2(s * (SCALE * LOG2E) - rows[b, 0:1, :])
        if diag:
            p = jnp.where(diag_mask(), p, 0.0)
        dp = lax.dot_general(vv, dd, NT, preferred_element_type=F32)
        dv_acc[...] += jnp.dot(p.astype(BF16), dd, preferred_element_type=F32)
        ds = (p * (dp - rows[b, 1:2, :])).astype(BF16)
        dk_acc[...] += jnp.dot(ds, qq, preferred_element_type=F32)
        dqt = lax.dot_general(kk, ds, TN, preferred_element_type=F32)
        for y in range(2):
            part = dqt[:, y * KB:(y + 1) * KB]
            if diag:
                dq[b, y] = part
            else:
                dq[b, y] += part

    def send_kv(c):
        for i in range(1, CH):
            h = peer(i)
            rcopy(kvs.at[c, h], rkv.at[c, chip], s_kv.at[c], r_kv.at[c], dev(h)).start()

    def make_kv(c):
        kvs[c, :, 0] = (dk_acc[...] * SCALE).astype(BF16).reshape(CH, R, D)
        kvs[c, :, 1] = dv_acc[...].astype(BF16).reshape(CH, R, D)
        rkv[c, chip] = kvs[c, chip]

    def step(n):
        c = C - 1 - n
        forwarded(c).wait_recv()
        clear()
        whole = n // U
        loop(0, whole, lambda u: [tile(c, c + 1 + U * u + x, False) for x in range(U)])
        loop(c + 1 + whole * U, C, lambda b: tile(c, b, False))
        arrive(c - 1)
        tile(c, c, True)
        make_kv(c)
        send_kv(c)

    loop(0, C - 1, step)

    def swap(b):
        rcopy(dq.at[b, 1 - core], dqin.at[b], s_x.at[b], r_x.at[b], sib).start()

    def give_q(b):
        rcopy(dq.at[b, core], dqin.at[b], s_x.at[b], r_x.at[b], sib).wait_recv()
        dqs[b] = ((dq[b, core] + dqin[b]) * SCALE).T.astype(BF16).reshape(CH, R, D)
        rq[b, chip] = dqs[b, chip]
        for i in range(1, CH):
            h = peer(i)
            rcopy(dqs.at[b, h], rq.at[b, chip], s_q.at[b], r_q.at[b], dev(h)).start()

    forwarded(0).wait_recv()
    clear()
    tile(0, 0, True)
    tile(0, 1, False)
    swap(0)
    swap(1)

    def last(u):
        tile(0, 2 * u, False)
        tile(0, 2 * u + 1, False)
        swap(2 * u)
        swap(2 * u + 1)

        @pl.when(u >= 2)
        def _():
            give_q(2 * u - 4)
            give_q(2 * u - 3)

    loop(1, C // 2, last)
    make_kv(0)
    send_kv(0)
    loop(C - 4, C, give_q)

    def put_kv(n):
        c = C - 1 - n
        rcopy(kvs.at[c, pl.ds(0, CH - 1)], rkv.at[c, pl.ds(0, CH - 1)], s_kv.at[c], r_kv.at[c], sib).wait_recv()
        for t, ref in enumerate((dk_out, dv_out)):
            for h in range(CH):
                tmp[t, pl.ds(h, R, stride=CH), :] = rkv[c, h, t].astype(F32)
            ref[pl.ds(pl.multiple_of(c * KB, KB), KB), :] = tmp[t].astype(BF16)

    loop(0, C, put_kv)

    def put_q(c):
        rcopy(dqs.at[c, pl.ds(0, CH - 1)], rq.at[c, pl.ds(0, CH - 1)], s_q.at[c], r_q.at[c], sib).wait_recv()
        for h in range(CH):
            tmp[2, pl.ds(h, R, stride=CH), :] = rq[c, h].astype(F32)
        dq_out[pl.ds(pl.multiple_of(c * KB, KB), KB), :] = tmp[2].astype(BF16)

    def drain(c):
        rcopy(stage.at[c, pl.ds(0, CH - 1)], buf.at[c, core, pl.ds(0, CH - 1)], s_in.at[c], r_in.at[c], sib).wait_send()
        forwarded(c).wait_send()
        rcopy(kvs.at[c, pl.ds(0, CH - 1)], rkv.at[c, pl.ds(0, CH - 1)], s_kv.at[c], r_kv.at[c], sib).wait_send()
        rcopy(dq.at[c, core], dqin.at[c], s_x.at[c], r_x.at[c], sib).wait_send()

    def drain_q(c):
        rcopy(dqs.at[c, pl.ds(0, CH - 1)], rq.at[c, pl.ds(0, CH - 1)], s_q.at[c], r_q.at[c], sib).wait_send()

    rcopy(statbuf.at[core, pl.ds(0, CH - 1)], statbuf.at[core, pl.ds(0, CH - 1)],
          s_st.at[0], r_st.at[0], sib).wait_send()
    fst.wait_send()
    loop(0, C, put_q)
    loop(0, C, drain)
    loop(0, C, drain_q)


def _write(dq_ref, dk_ref, dv_ref, dq_hbm, dk_hbm, dv_hbm, sem):
    copies = [pltpu.make_async_copy(a, b, sem.at[i])
              for i, (a, b) in enumerate(((dq_ref, dq_hbm), (dk_ref, dk_hbm), (dv_ref, dv_hbm)))]
    for x in copies:
        x.start()
    for x in copies:
        x.wait()


def solution(mesh):
    rows = P(('data', 'cp'))
    cols = P(None, ('data', 'cp'))

    def local(q, k, v, o, dout, lse):
        c, h, d = q.shape
        flat = lambda x: x.reshape(c * h, d)
        vm = pl.BlockSpec(memory_space=pltpu.VMEM)
        hbm = pl.BlockSpec(memory_space=pltpu.HBM)
        sem = pltpu.SemaphoreType.DMA
        outs = pl.pallas_call(
            _kernel,
            out_shape=[pltpu.VMEM((c * h, d), BF16)] * 3,
            in_specs=[hbm] * 6,
            out_specs=[vm] * 3,
            scratch_shapes=[
                pltpu.VMEM((5, c * h, d), BF16),
                pltpu.VMEM((h, c), F32),
                pltpu.VMEM((C, CH, 4, R, D), BF16),
                pltpu.VMEM((C, CH, R, D), BF16),
                pltpu.VMEM((CH, 1, 2 * c), F32),
                pltpu.VMEM((C, 2, CH, 4, R, D), BF16),
                pltpu.VMEM((2, CH, 1, 2 * c), F32),
                pltpu.VMEM((C, 8, QB), F32),
                pltpu.VMEM((C, 2, D, KB), F32),
                pltpu.VMEM((C, D, KB), F32),
                pltpu.VMEM((C, CH, R, D), BF16),
                pltpu.VMEM((C, CH, 2, R, D), BF16),
                pltpu.VMEM((C, CH, 2, R, D), BF16),
                pltpu.VMEM((C, CH, R, D), BF16),
                pltpu.VMEM((5, KB, D), F32),
                pltpu.VMEM((KB, D), F32),
                pltpu.VMEM((KB, D), F32),
            ] + [sem((C,))] * 10 + [sem((2,))] * 2 + [sem((2, 5))],
            compiler_params=pltpu.CompilerParams(collective_id=0, has_side_effects=True,
                                                 vmem_limit_bytes=40 * 2 ** 20),
        )(*[pltpu.with_memory_space_constraint(x, pltpu.HBM) for x in (flat(k), flat(v), flat(q), flat(dout), flat(o), lse)])
        outs = pl.pallas_call(
            _write,
            out_shape=[jax.ShapeDtypeStruct((c * h, d), BF16)] * 3,
            in_specs=[vm] * 3,
            out_specs=[hbm] * 3,
            scratch_shapes=[sem((3,))],
            compiler_params=pltpu.CompilerParams(vmem_limit_bytes=2 ** 20),
        )(*[pltpu.with_memory_space_constraint(x, pltpu.VMEM) for x in outs])
        return tuple(x.reshape(c, h, d) for x in outs)

    return jax.shard_map(local, mesh=mesh, in_specs=(rows, rows, rows, rows, rows, cols),
                         out_specs=(rows, rows, rows), check_vma=False)
```

```python
import functools
import math

import jax
import jax.numpy as jnp
from jax import lax
from jax.experimental import pallas as pl
from jax.experimental.pallas import tpu as pltpu
from jax.sharding import PartitionSpec as P

MESH = pl.DeviceIdType.MESH
F32 = jnp.float32
BF16 = jnp.bfloat16

CH = 8
R = 32
C = 16
KB = CH * R
QB = 2 * KB
D = 128
NT = (((1,), (1,)), ((), ()))
TN = (((0,), (0,)), ((), ()))
LOG2E = math.log2(math.e)
U = 4
GK = 2
GQ = 4
SCALE = D ** -0.5


def _kernel(k_hbm, v_hbm, q_hbm, do_hbm, o_hbm, lse_hbm, dq_out, dk_out, dv_out,
            xin, lsev, stage, ostage, statloc, buf, statbuf, rows, dq, dqin, dqs, kvs, rkv, rq, tmp, dk_acc, dv_acc,
            s_in, r_in, s_fw, r_fw, s_kv, r_kv, s_x, r_x, s_q, r_q, s_st, r_st, s_ld):
    cp = lax.axis_index('cp')
    chip = cp // 2
    core = cp % 2
    sib = {'cp': chip * 2 + 1 - core}

    hbm = (k_hbm, v_hbm, q_hbm, do_hbm, o_hbm)
    lead = (C - 1) * KB
    loads = []
    for t in range(4):
        loads.append(pltpu.make_async_copy(hbm[t].at[pl.ds(lead, KB)], xin.at[t, pl.ds(lead, KB)], s_ld.at[0, t]))
    for t in range(4):
        loads.append(pltpu.make_async_copy(hbm[t].at[pl.ds(0, lead)], xin.at[t, pl.ds(0, lead)], s_ld.at[1, t]))
    loads.append(pltpu.make_async_copy(o_hbm, xin.at[4], s_ld.at[0, 4]))
    loads.append(pltpu.make_async_copy(lse_hbm, lsev, s_ld.at[1, 4]))
    for x in loads:
        x.start()

    def peer(i):
        return lax.rem(chip + i, CH)

    def dev(h):
        return {'cp': h * 2 + core}

    def rcopy(src, dst, ss, rs, to):
        return pltpu.make_async_remote_copy(src_ref=src, dst_ref=dst, send_sem=ss, recv_sem=rs,
                                            device_id=to, device_id_type=MESH)

    def gather(c):
        r0 = pl.multiple_of(c * KB, KB)
        for t in range(4):
            tmp[t] = xin[t, pl.ds(r0, KB), :].astype(F32)
            for h in range(CH):
                stage[c, h, t] = tmp[t, pl.ds(h, R, stride=CH), :].astype(BF16)
        buf[c, core, chip] = stage[c, chip]

    def gather_o(c):
        tmp[4] = xin[4, pl.ds(pl.multiple_of(c * KB, KB), KB), :].astype(F32)
        for h in range(CH):
            ostage[c, h] = tmp[4, pl.ds(h, R, stride=CH), :].astype(BF16)

    def send(c):
        for i in range(1, CH):
            h = peer(i)
            rcopy(stage.at[c, h], buf.at[c, core, chip], s_in.at[c], r_in.at[c], dev(h)).start()

    def loop(lo, hi, f):
        lax.fori_loop(lo, hi, lambda x, _: (f(x), 0)[1], 0)

    barrier = pltpu.get_barrier_semaphore()
    pl.semaphore_signal(barrier, inc=1, device_id=sib, device_id_type=MESH)
    for i in range(1, CH):
        pl.semaphore_signal(barrier, inc=1, device_id=dev(peer(i)), device_id_type=MESH)
    for x in loads[:4]:
        x.wait()
    gather(C - 1)
    pl.semaphore_wait(barrier, CH)
    send(C - 1)
    for x in loads[4:]:
        x.wait()
    gather(C - 2)
    gather(C - 3)
    send(C - 2)
    gather(C - 4)
    send(C - 3)
    loop(0, C - 4, lambda n: gather(C - 5 - n))
    send(C - 4)
    loop(0, C, gather_o)

    ones = jnp.ones((8, D), BF16)
    for h in range(CH):
        x = (stage[:, h, 3].astype(F32) * ostage[:, h].astype(F32)).reshape(C * R, D)
        hi = x.astype(BF16)
        lo = (x - hi.astype(F32)).astype(BF16)
        e = (lax.dot_general(ones, hi, NT, preferred_element_type=F32)
             + lax.dot_general(ones, lo, NT, preferred_element_type=F32))
        statloc[h, :, :C * R] = lsev[h:h + 1, :]
        statloc[h, :, C * R:] = e[0:1, :]
    statbuf[core, chip] = statloc[chip]
    for i in range(1, CH):
        h = peer(i)
        rcopy(statloc.at[h], statbuf.at[core, chip], s_st.at[0], r_st.at[0], dev(h)).start()
    loop(0, C - 4, lambda n: send(C - 5 - n))

    def arrive(c):
        rcopy(buf.at[c, core, pl.ds(0, CH - 1)], buf.at[c, core, pl.ds(0, CH - 1)],
              s_in.at[c], r_in.at[c], sib).wait_recv()
        rcopy(buf.at[c, core, :, pl.ds(2, 2)], buf.at[c, core, :, pl.ds(2, 2)],
              s_fw.at[c], r_fw.at[c], sib).start()

    def forwarded(c):
        return rcopy(buf.at[c, 1 - core, :, pl.ds(2, 2)], buf.at[c, 1 - core, :, pl.ds(2, 2)],
                     s_fw.at[c], r_fw.at[c], sib)

    arrive(C - 1)
    rcopy(statbuf.at[core, pl.ds(0, CH - 1)], statbuf.at[core, pl.ds(0, CH - 1)],
          s_st.at[0], r_st.at[0], sib).wait_recv()
    fst = rcopy(statbuf.at[core], statbuf.at[core], s_st.at[1], r_st.at[1], sib)
    fst.start()
    rcopy(statbuf.at[1 - core], statbuf.at[1 - core], s_st.at[1], r_st.at[1], sib).wait_recv()
    quarter = lax.broadcasted_iota(jnp.int32, (1, 128), 1) // R
    for st in range(2):
        mul = LOG2E if st == 0 else 1.0
        for t in range(4):
            for g in range(4):
                src = [statbuf[g // 2, (g % 2) * 4 + m, :, st * 512 + t * 128:st * 512 + t * 128 + 128] * mul
                       for m in range(4)]
                for r in range(4):
                    acc = jnp.zeros((1, 128), F32)
                    for m in range(4):
                        sh = ((m - r) % 4) * R
                        x = pltpu.roll(src[m], sh, 1) if sh else src[m]
                        acc = jnp.where(quarter == m, x, acc)
                    rows[4 * t + r, st:st + 1, g * 128:(g + 1) * 128] = acc

    def diag_mask():
        ki = lax.broadcasted_iota(jnp.int32, (KB, QB), 0)
        qi = lax.broadcasted_iota(jnp.int32, (KB, QB), 1)
        kpos = (ki % R) * 16 + (ki // R) * 2 + core
        qpos = (qi % R) * 16 + ((qi // R) % CH) * 2 + qi // KB
        return kpos <= qpos

    def clear():
        dk_acc[...] = jnp.zeros_like(dk_acc)
        dv_acc[...] = jnp.zeros_like(dv_acc)

    def tile(c, b, diag):
        kk = buf[c, core, :, 0].reshape(KB, D)
        vv = buf[c, core, :, 1].reshape(KB, D)
        qq = buf[b, :, :, 2].reshape(QB, D)
        dd = buf[b, :, :, 3].reshape(QB, D)
        s = lax.dot_general(kk, qq, NT, preferred_element_type=F32)
        p = jnp.exp2(s * (SCALE * LOG2E) - rows[b, 0:1, :])
        if diag:
            p = jnp.where(diag_mask(), p, 0.0)
        dp = lax.dot_general(vv, dd, NT, preferred_element_type=F32)
        dv_acc[...] += jnp.dot(p.astype(BF16), dd, preferred_element_type=F32)
        ds = (p * (dp - rows[b, 1:2, :])).astype(BF16)
        dk_acc[...] += jnp.dot(ds, qq, preferred_element_type=F32)
        dqt = lax.dot_general(kk, ds, TN, preferred_element_type=F32)
        for y in range(2):
            part = dqt[:, y * KB:(y + 1) * KB]
            if diag:
                dq[b, y] = part
            else:
                dq[b, y] += part

    def send_kv(g):
        for i in range(1, CH):
            h = peer(i)
            rcopy(kvs.at[g, h], rkv.at[g, chip], s_kv.at[g], r_kv.at[g], dev(h)).start()

    def make_kv(c):
        g = c // GK
        x = c % GK
        kvs[g, :, x, 0] = (dk_acc[...] * SCALE).astype(BF16).reshape(CH, R, D)
        kvs[g, :, x, 1] = dv_acc[...].astype(BF16).reshape(CH, R, D)
        rkv[g, chip, x] = kvs[g, chip, x]

    def step(n):
        c = C - 1 - n
        forwarded(c).wait_recv()
        clear()
        whole = n // U
        loop(0, whole, lambda u: [tile(c, c + 1 + U * u + x, False) for x in range(U)])
        loop(c + 1 + whole * U, C, lambda b: tile(c, b, False))
        arrive(c - 1)
        tile(c, c, True)
        make_kv(c)

        @pl.when(c % GK == 0)
        def _():
            send_kv(c // GK)

    loop(0, C - 1, step)

    def swap(b):
        rcopy(dq.at[b, 1 - core], dqin.at[b], s_x.at[b], r_x.at[b], sib).start()

    def give_q(b):
        rcopy(dq.at[b, core], dqin.at[b], s_x.at[b], r_x.at[b], sib).wait_recv()
        g = b // GQ
        x = b % GQ
        dqs[g, :, x] = ((dq[b, core] + dqin[b]) * SCALE).T.astype(BF16).reshape(CH, R, D)
        rq[g, chip, x] = dqs[g, chip, x]

    def send_q(g):
        for i in range(1, CH):
            h = peer(i)
            rcopy(dqs.at[g, h], rq.at[g, chip], s_q.at[g], r_q.at[g], dev(h)).start()

    forwarded(0).wait_recv()
    clear()
    tile(0, 0, True)
    tile(0, 1, False)
    swap(0)
    swap(1)

    def last(u):
        tile(0, 2 * u, False)
        tile(0, 2 * u + 1, False)
        swap(2 * u)
        swap(2 * u + 1)

        @pl.when(u >= 2)
        def _():
            give_q(2 * u - 4)
            give_q(2 * u - 3)

        @pl.when((u >= 2) & ((2 * u - 2) % GQ == 0))
        def _():
            send_q((2 * u - 2) // GQ - 1)

    loop(1, C // 2, last)
    make_kv(0)
    send_kv(0)
    loop(C - 4, C, give_q)
    loop((C - 4) // GQ, C // GQ, send_q)

    def all_kv(g):
        return rcopy(kvs.at[g, pl.ds(0, CH - 1)], rkv.at[g, pl.ds(0, CH - 1)], s_kv.at[g], r_kv.at[g], sib)

    def all_q(g):
        return rcopy(dqs.at[g, pl.ds(0, CH - 1)], rq.at[g, pl.ds(0, CH - 1)], s_q.at[g], r_q.at[g], sib)

    def put_kv(n):
        g = C // GK - 1 - n
        all_kv(g).wait_recv()
        for x in range(GK):
            for t, ref in enumerate((dk_out, dv_out)):
                for h in range(CH):
                    tmp[t, pl.ds(h, R, stride=CH), :] = rkv[g, h, x, t].astype(F32)
                ref[pl.ds(pl.multiple_of((g * GK + x) * KB, KB), KB), :] = tmp[t].astype(BF16)

    loop(0, C // GK, put_kv)

    def put_q(g):
        all_q(g).wait_recv()
        for x in range(GQ):
            for h in range(CH):
                tmp[x, pl.ds(h, R, stride=CH), :] = rq[g, h, x].astype(F32)
            dq_out[pl.ds(pl.multiple_of((g * GQ + x) * KB, KB), KB), :] = tmp[x].astype(BF16)

    def drain(c):
        rcopy(stage.at[c, pl.ds(0, CH - 1)], buf.at[c, core, pl.ds(0, CH - 1)], s_in.at[c], r_in.at[c], sib).wait_send()
        forwarded(c).wait_send()
        rcopy(dq.at[c, core], dqin.at[c], s_x.at[c], r_x.at[c], sib).wait_send()

    rcopy(statbuf.at[core, pl.ds(0, CH - 1)], statbuf.at[core, pl.ds(0, CH - 1)],
          s_st.at[0], r_st.at[0], sib).wait_send()
    fst.wait_send()
    loop(0, C, drain)
    loop(0, C // GQ, put_q)
    loop(0, C // GK, lambda g: all_kv(g).wait_send())
    loop(0, C // GQ, lambda g: all_q(g).wait_send())


def _write(dq_ref, dk_ref, dv_ref, dq_hbm, dk_hbm, dv_hbm, sem):
    copies = [pltpu.make_async_copy(a, b, sem.at[i])
              for i, (a, b) in enumerate(((dq_ref, dq_hbm), (dk_ref, dk_hbm), (dv_ref, dv_hbm)))]
    for x in copies:
        x.start()
    for x in copies:
        x.wait()


def solution(mesh):
    rows = P(('data', 'cp'))
    cols = P(None, ('data', 'cp'))

    def local(q, k, v, o, dout, lse):
        c, h, d = q.shape
        flat = lambda x: x.reshape(c * h, d)
        vm = pl.BlockSpec(memory_space=pltpu.VMEM)
        hbm = pl.BlockSpec(memory_space=pltpu.HBM)
        sem = pltpu.SemaphoreType.DMA
        outs = pl.pallas_call(
            _kernel,
            out_shape=[pltpu.VMEM((c * h, d), BF16)] * 3,
            in_specs=[hbm] * 6,
            out_specs=[vm] * 3,
            scratch_shapes=[
                pltpu.VMEM((5, c * h, d), BF16),
                pltpu.VMEM((h, c), F32),
                pltpu.VMEM((C, CH, 4, R, D), BF16),
                pltpu.VMEM((C, CH, R, D), BF16),
                pltpu.VMEM((CH, 1, 2 * c), F32),
                pltpu.VMEM((C, 2, CH, 4, R, D), BF16),
                pltpu.VMEM((2, CH, 1, 2 * c), F32),
                pltpu.VMEM((C, 8, QB), F32),
                pltpu.VMEM((C, 2, D, KB), F32),
                pltpu.VMEM((C, D, KB), F32),
                pltpu.VMEM((C // GQ, CH, GQ, R, D), BF16),
                pltpu.VMEM((C // GK, CH, GK, 2, R, D), BF16),
                pltpu.VMEM((C // GK, CH, GK, 2, R, D), BF16),
                pltpu.VMEM((C // GQ, CH, GQ, R, D), BF16),
                pltpu.VMEM((5, KB, D), F32),
                pltpu.VMEM((KB, D), F32),
                pltpu.VMEM((KB, D), F32),
            ] + [sem((C,))] * 10 + [sem((2,))] * 2 + [sem((2, 5))],
            compiler_params=pltpu.CompilerParams(collective_id=0, has_side_effects=True,
                                                 vmem_limit_bytes=40 * 2 ** 20),
        )(*[pltpu.with_memory_space_constraint(x, pltpu.HBM) for x in (flat(k), flat(v), flat(q), flat(dout), flat(o), lse)])
        outs = pl.pallas_call(
            _write,
            out_shape=[jax.ShapeDtypeStruct((c * h, d), BF16)] * 3,
            in_specs=[vm] * 3,
            out_specs=[hbm] * 3,
            scratch_shapes=[sem((3,))],
            compiler_params=pltpu.CompilerParams(vmem_limit_bytes=2 ** 20),
        )(*[pltpu.with_memory_space_constraint(x, pltpu.VMEM) for x in outs])
        return tuple(x.reshape(c, h, d) for x in outs)

    return jax.shard_map(local, mesh=mesh, in_specs=(rows, rows, rows, rows, rows, cols),
                         out_specs=(rows, rows, rows), check_vma=False)
```

```python
import functools
import math

import jax
import jax.numpy as jnp
from jax import lax
from jax.experimental import pallas as pl
from jax.experimental.pallas import tpu as pltpu
from jax.sharding import PartitionSpec as P

MESH = pl.DeviceIdType.MESH
F32 = jnp.float32
BF16 = jnp.bfloat16

CH = 8
R = 32
C = 16
KB = CH * R
QB = 2 * KB
D = 128
NT = (((1,), (1,)), ((), ()))
TN = (((0,), (0,)), ((), ()))
LOG2E = math.log2(math.e)
U = 4
GK = 4
GQ = 4
SCALE = D ** -0.5


def _kernel(k_hbm, v_hbm, q_hbm, do_hbm, o_hbm, lse_hbm, dq_out, dk_out, dv_out,
            xin, lsev, stage, ostage, statloc, buf, statbuf, rows, dq, dqin, dqs, kvs, rkv, rq, tmp, dk_acc, dv_acc,
            s_in, r_in, s_fw, r_fw, s_kv, r_kv, s_x, r_x, s_q, r_q, s_st, r_st, s_ld, two, three):
    cp = lax.axis_index('cp')
    chip = cp // 2
    core = cp % 2
    sib = {'cp': chip * 2 + 1 - core}

    hbm = (k_hbm, v_hbm, q_hbm, do_hbm, o_hbm)
    lead = (C - 1) * KB
    loads = []
    for t in range(4):
        loads.append(pltpu.make_async_copy(hbm[t].at[pl.ds(lead, KB)], xin.at[t, pl.ds(lead, KB)], s_ld.at[0, t]))
    for t in range(4):
        loads.append(pltpu.make_async_copy(hbm[t].at[pl.ds(0, lead)], xin.at[t, pl.ds(0, lead)], s_ld.at[1, t]))
    loads.append(pltpu.make_async_copy(o_hbm, xin.at[4], s_ld.at[0, 4]))
    loads.append(pltpu.make_async_copy(lse_hbm, lsev, s_ld.at[1, 4]))
    for x in loads:
        x.start()

    def peer(i):
        return lax.rem(chip + CH + jnp.where(chip < CH // 2, i, -i), CH)

    def dev(h):
        return {'cp': h * 2 + core}

    def rcopy(src, dst, ss, rs, to):
        return pltpu.make_async_remote_copy(src_ref=src, dst_ref=dst, send_sem=ss, recv_sem=rs,
                                            device_id=to, device_id_type=MESH)

    def gather(c):
        r0 = pl.multiple_of(c * KB, KB)
        for t in range(4):
            tmp[t] = xin[t, pl.ds(r0, KB), :].astype(F32)
            for h in range(CH):
                stage[c, h, t] = tmp[t, pl.ds(h, R, stride=CH), :].astype(BF16)
        buf[c, core, chip] = stage[c, chip]

    def gather_o(c):
        tmp[4] = xin[4, pl.ds(pl.multiple_of(c * KB, KB), KB), :].astype(F32)
        for h in range(CH):
            ostage[c, h] = tmp[4, pl.ds(h, R, stride=CH), :].astype(BF16)

    def send_one(c, h):
        rcopy(stage.at[c, h], buf.at[c, core, chip], s_in.at[c], r_in.at[c], dev(h)).start()

    def send(c):
        for i in range(CH - 1, 0, -1):
            send_one(c, peer(i))

    z = chip // 2
    inner = z * (3 - z) // 2

    def far(h):
        return (h // 2 - z) * (h // 2 - z)

    def send_at(c, dist):
        for i in range(CH - 1, 0, -1):
            h = peer(i)

            @pl.when(far(h) <= 1 if dist == 1 else far(h) == dist * dist)
            def _():
                send_one(c, h)

    def tell(sem, zz):
        pl.semaphore_signal(sem, inc=1, device_id=dev(zz * 2 + chip % 2), device_id_type=MESH)

    def loop(lo, hi, f):
        lax.fori_loop(lo, hi, lambda x, _: (f(x), 0)[1], 0)

    barrier = pltpu.get_barrier_semaphore()
    pl.semaphore_signal(barrier, inc=1, device_id=sib, device_id_type=MESH)
    for i in range(CH - 1, 0, -1):
        h = peer(i)

        @pl.when(far(h) <= 1)
        def _():
            pl.semaphore_signal(barrier, inc=1, device_id=dev(h), device_id_type=MESH)
    for x in loads[:4]:
        x.wait()
    gather(C - 1)
    pl.semaphore_wait(barrier, 4 + 2 * inner)

    @pl.when(inner == 1)
    def _():
        tell(two, 3 - z)
        tell(two, 3 * (z - 1))
    send_at(C - 1, 1)
    pl.semaphore_wait(two, 1)

    @pl.when(inner == 1)
    def _():
        tell(three, 3 * (z - 1))
    send_at(C - 1, 2)

    @pl.when(inner == 0)
    def _():
        pl.semaphore_wait(three, 1)
    send_at(C - 1, 3)
    for x in loads[4:]:
        x.wait()
    gather(C - 2)
    gather(C - 3)
    send(C - 2)
    gather(C - 4)
    send(C - 3)
    loop(0, C - 4, lambda n: gather(C - 5 - n))
    send(C - 4)
    loop(0, C, gather_o)

    ones = jnp.ones((8, D), BF16)
    for h in range(CH):
        x = (stage[:, h, 3].astype(F32) * ostage[:, h].astype(F32)).reshape(C * R, D)
        hi = x.astype(BF16)
        lo = (x - hi.astype(F32)).astype(BF16)
        e = (lax.dot_general(ones, hi, NT, preferred_element_type=F32)
             + lax.dot_general(ones, lo, NT, preferred_element_type=F32))
        statloc[h, :, :C * R] = lsev[h:h + 1, :]
        statloc[h, :, C * R:] = e[0:1, :]
    statbuf[core, chip] = statloc[chip]
    for i in range(CH - 1, 0, -1):
        h = peer(i)
        rcopy(statloc.at[h], statbuf.at[core, chip], s_st.at[0], r_st.at[0], dev(h)).start()
    loop(0, C - 4, lambda n: send(C - 5 - n))

    def arrive(c):
        rcopy(buf.at[c, core, pl.ds(0, CH - 1)], buf.at[c, core, pl.ds(0, CH - 1)],
              s_in.at[c], r_in.at[c], sib).wait_recv()
        rcopy(buf.at[c, core, :, pl.ds(2, 2)], buf.at[c, core, :, pl.ds(2, 2)],
              s_fw.at[c], r_fw.at[c], sib).start()

    def forwarded(c):
        return rcopy(buf.at[c, 1 - core, :, pl.ds(2, 2)], buf.at[c, 1 - core, :, pl.ds(2, 2)],
                     s_fw.at[c], r_fw.at[c], sib)

    arrive(C - 1)
    rcopy(statbuf.at[core, pl.ds(0, CH - 1)], statbuf.at[core, pl.ds(0, CH - 1)],
          s_st.at[0], r_st.at[0], sib).wait_recv()
    fst = rcopy(statbuf.at[core], statbuf.at[core], s_st.at[1], r_st.at[1], sib)
    fst.start()
    rcopy(statbuf.at[1 - core], statbuf.at[1 - core], s_st.at[1], r_st.at[1], sib).wait_recv()
    quarter = lax.broadcasted_iota(jnp.int32, (1, 128), 1) // R
    for st in range(2):
        mul = LOG2E if st == 0 else 1.0
        for t in range(4):
            for g in range(4):
                src = [statbuf[g // 2, (g % 2) * 4 + m, :, st * 512 + t * 128:st * 512 + t * 128 + 128] * mul
                       for m in range(4)]
                for r in range(4):
                    acc = jnp.zeros((1, 128), F32)
                    for m in range(4):
                        sh = ((m - r) % 4) * R
                        x = pltpu.roll(src[m], sh, 1) if sh else src[m]
                        acc = jnp.where(quarter == m, x, acc)
                    rows[4 * t + r, st:st + 1, g * 128:(g + 1) * 128] = acc

    def diag_mask():
        ki = lax.broadcasted_iota(jnp.int32, (KB, QB), 0)
        qi = lax.broadcasted_iota(jnp.int32, (KB, QB), 1)
        kpos = (ki % R) * 16 + (ki // R) * 2 + core
        qpos = (qi % R) * 16 + ((qi // R) % CH) * 2 + qi // KB
        return kpos <= qpos

    def clear():
        dk_acc[...] = jnp.zeros_like(dk_acc)
        dv_acc[...] = jnp.zeros_like(dv_acc)

    def tile(c, b, diag):
        kk = buf[c, core, :, 0].reshape(KB, D)
        vv = buf[c, core, :, 1].reshape(KB, D)
        qq = buf[b, :, :, 2].reshape(QB, D)
        dd = buf[b, :, :, 3].reshape(QB, D)
        s = lax.dot_general(kk, qq, NT, preferred_element_type=F32)
        p = jnp.exp2(s * (SCALE * LOG2E) - rows[b, 0:1, :])
        if diag:
            p = jnp.where(diag_mask(), p, 0.0)
        dp = lax.dot_general(vv, dd, NT, preferred_element_type=F32)
        dv_acc[...] += jnp.dot(p.astype(BF16), dd, preferred_element_type=F32)
        ds = (p * (dp - rows[b, 1:2, :])).astype(BF16)
        dk_acc[...] += jnp.dot(ds, qq, preferred_element_type=F32)
        dqt = lax.dot_general(kk, ds, TN, preferred_element_type=F32)
        for y in range(2):
            part = dqt[:, y * KB:(y + 1) * KB]
            if diag:
                dq[b, y] = part
            else:
                dq[b, y] += part

    def send_kv(g):
        for i in range(CH - 1, 0, -1):
            h = peer(i)
            rcopy(kvs.at[g, h], rkv.at[g, chip], s_kv.at[g], r_kv.at[g], dev(h)).start()

    def make_kv(c):
        g = c // GK
        x = c % GK
        kvs[g, :, x, 0] = (dk_acc[...] * SCALE).astype(BF16).reshape(CH, R, D)
        kvs[g, :, x, 1] = dv_acc[...].astype(BF16).reshape(CH, R, D)
        rkv[g, chip, x] = kvs[g, chip, x]

    def step(n):
        c = C - 1 - n
        forwarded(c).wait_recv()
        clear()
        whole = n // U
        loop(0, whole, lambda u: [tile(c, c + 1 + U * u + x, False) for x in range(U)])
        loop(c + 1 + whole * U, C, lambda b: tile(c, b, False))
        arrive(c - 1)
        tile(c, c, True)
        make_kv(c)

        @pl.when(c % GK == 0)
        def _():
            send_kv(c // GK)

    loop(0, C - 1, step)

    def swap(b):
        rcopy(dq.at[b, 1 - core], dqin.at[b], s_x.at[b], r_x.at[b], sib).start()

    def give_q(b):
        rcopy(dq.at[b, core], dqin.at[b], s_x.at[b], r_x.at[b], sib).wait_recv()
        g = b // GQ
        x = b % GQ
        dqs[g, :, x] = ((dq[b, core] + dqin[b]) * SCALE).T.astype(BF16).reshape(CH, R, D)
        rq[g, chip, x] = dqs[g, chip, x]

    def send_q(g):
        for i in range(CH - 1, 0, -1):
            h = peer(i)
            rcopy(dqs.at[g, h], rq.at[g, chip], s_q.at[g], r_q.at[g], dev(h)).start()

    forwarded(0).wait_recv()
    clear()
    tile(0, 0, True)
    tile(0, 1, False)
    swap(0)
    swap(1)

    def last(u):
        tile(0, 2 * u, False)
        tile(0, 2 * u + 1, False)
        swap(2 * u)
        swap(2 * u + 1)

        @pl.when(u >= 2)
        def _():
            give_q(2 * u - 4)
            give_q(2 * u - 3)

        @pl.when((u >= 2) & ((2 * u - 2) % GQ == 0))
        def _():
            send_q((2 * u - 2) // GQ - 1)

    loop(1, C // 2, last)
    make_kv(0)
    send_kv(0)
    loop(C - 4, C, give_q)
    loop((C - 4) // GQ, C // GQ, send_q)

    def all_kv(g):
        return rcopy(kvs.at[g, pl.ds(0, CH - 1)], rkv.at[g, pl.ds(0, CH - 1)], s_kv.at[g], r_kv.at[g], sib)

    def all_q(g):
        return rcopy(dqs.at[g, pl.ds(0, CH - 1)], rq.at[g, pl.ds(0, CH - 1)], s_q.at[g], r_q.at[g], sib)

    def put_kv(n):
        g = C // GK - 1 - n
        all_kv(g).wait_recv()
        for x in range(GK):
            for t, ref in enumerate((dk_out, dv_out)):
                for h in range(CH):
                    tmp[t, pl.ds(h, R, stride=CH), :] = rkv[g, h, x, t].astype(F32)
                ref[pl.ds(pl.multiple_of((g * GK + x) * KB, KB), KB), :] = tmp[t].astype(BF16)

    loop(0, C // GK, put_kv)

    def put_q(g):
        all_q(g).wait_recv()
        for x in range(GQ):
            for h in range(CH):
                tmp[x, pl.ds(h, R, stride=CH), :] = rq[g, h, x].astype(F32)
            dq_out[pl.ds(pl.multiple_of((g * GQ + x) * KB, KB), KB), :] = tmp[x].astype(BF16)

    def drain(c):
        rcopy(stage.at[c, pl.ds(0, CH - 1)], buf.at[c, core, pl.ds(0, CH - 1)], s_in.at[c], r_in.at[c], sib).wait_send()
        forwarded(c).wait_send()
        rcopy(dq.at[c, core], dqin.at[c], s_x.at[c], r_x.at[c], sib).wait_send()

    rcopy(statbuf.at[core, pl.ds(0, CH - 1)], statbuf.at[core, pl.ds(0, CH - 1)],
          s_st.at[0], r_st.at[0], sib).wait_send()
    fst.wait_send()
    loop(0, C, drain)
    loop(0, C // GQ, put_q)
    loop(0, C // GK, lambda g: all_kv(g).wait_send())
    loop(0, C // GQ, lambda g: all_q(g).wait_send())


def _write(dq_ref, dk_ref, dv_ref, dq_hbm, dk_hbm, dv_hbm, sem):
    copies = [pltpu.make_async_copy(a, b, sem.at[i])
              for i, (a, b) in enumerate(((dq_ref, dq_hbm), (dk_ref, dk_hbm), (dv_ref, dv_hbm)))]
    for x in copies:
        x.start()
    for x in copies:
        x.wait()


def solution(mesh):
    rows = P(('data', 'cp'))
    cols = P(None, ('data', 'cp'))

    def local(q, k, v, o, dout, lse):
        c, h, d = q.shape
        flat = lambda x: x.reshape(c * h, d)
        vm = pl.BlockSpec(memory_space=pltpu.VMEM)
        hbm = pl.BlockSpec(memory_space=pltpu.HBM)
        sem = pltpu.SemaphoreType.DMA
        outs = pl.pallas_call(
            _kernel,
            out_shape=[pltpu.VMEM((c * h, d), BF16)] * 3,
            in_specs=[hbm] * 6,
            out_specs=[vm] * 3,
            scratch_shapes=[
                pltpu.VMEM((5, c * h, d), BF16),
                pltpu.VMEM((h, c), F32),
                pltpu.VMEM((C, CH, 4, R, D), BF16),
                pltpu.VMEM((C, CH, R, D), BF16),
                pltpu.VMEM((CH, 1, 2 * c), F32),
                pltpu.VMEM((C, 2, CH, 4, R, D), BF16),
                pltpu.VMEM((2, CH, 1, 2 * c), F32),
                pltpu.VMEM((C, 8, QB), F32),
                pltpu.VMEM((C, 2, D, KB), F32),
                pltpu.VMEM((C, D, KB), F32),
                pltpu.VMEM((C // GQ, CH, GQ, R, D), BF16),
                pltpu.VMEM((C // GK, CH, GK, 2, R, D), BF16),
                pltpu.VMEM((C // GK, CH, GK, 2, R, D), BF16),
                pltpu.VMEM((C // GQ, CH, GQ, R, D), BF16),
                pltpu.VMEM((5, KB, D), F32),
                pltpu.VMEM((KB, D), F32),
                pltpu.VMEM((KB, D), F32),
            ] + [sem((C,))] * 10 + [sem((2,))] * 2 + [sem((2, 5))] + [pltpu.SemaphoreType.REGULAR] * 2,
            compiler_params=pltpu.CompilerParams(collective_id=0, has_side_effects=True,
                                                 vmem_limit_bytes=40 * 2 ** 20),
        )(*[pltpu.with_memory_space_constraint(x, pltpu.HBM) for x in (flat(k), flat(v), flat(q), flat(dout), flat(o), lse)])
        outs = pl.pallas_call(
            _write,
            out_shape=[jax.ShapeDtypeStruct((c * h, d), BF16)] * 3,
            in_specs=[vm] * 3,
            out_specs=[hbm] * 3,
            scratch_shapes=[sem((3,))],
            compiler_params=pltpu.CompilerParams(vmem_limit_bytes=2 ** 20),
        )(*[pltpu.with_memory_space_constraint(x, pltpu.VMEM) for x in outs])
        return tuple(x.reshape(c, h, d) for x in outs)

    return jax.shard_map(local, mesh=mesh, in_specs=(rows, rows, rows, rows, rows, cols),
                         out_specs=(rows, rows, rows), check_vma=False)
```

```python
import functools
import math

import jax
import jax.numpy as jnp
from jax import lax
from jax.experimental import pallas as pl
from jax.experimental.pallas import tpu as pltpu
from jax.sharding import PartitionSpec as P

MESH = pl.DeviceIdType.MESH
F32 = jnp.float32
BF16 = jnp.bfloat16

CH = 8
R = 32
C = 16
KB = CH * R
QB = 2 * KB
D = 128
NT = (((1,), (1,)), ((), ()))
TN = (((0,), (0,)), ((), ()))
LOG2E = math.log2(math.e)
U = 4
GK = 4
GQ = 4
SCALE = D ** -0.5


def _kernel(k_hbm, v_hbm, q_hbm, do_hbm, o_hbm, lse_hbm, dq_out, dk_out, dv_out,
            xin, lsev, stage, ostage, statloc, buf, statbuf, rows, dq, dqin, dqs, kvs, rkv, rq, tmp, dk_acc, dv_acc,
            s_in, r_in, s_fw, r_fw, s_kv, r_kv, s_x, r_x, s_q, r_q, s_st, r_st, s_ld, two, three):
    cp = lax.axis_index('cp')
    chip = cp // 2
    core = cp % 2
    sib = {'cp': chip * 2 + 1 - core}

    hbm = (k_hbm, v_hbm, q_hbm, do_hbm, o_hbm)
    lead = (C - 1) * KB
    loads = []
    for t in range(4):
        loads.append(pltpu.make_async_copy(hbm[t].at[pl.ds(lead, KB)], xin.at[t, pl.ds(lead, KB)], s_ld.at[0, t]))
    for t in range(4):
        loads.append(pltpu.make_async_copy(hbm[t].at[pl.ds(0, lead)], xin.at[t, pl.ds(0, lead)], s_ld.at[1, t]))
    loads.append(pltpu.make_async_copy(o_hbm, xin.at[4], s_ld.at[0, 4]))
    loads.append(pltpu.make_async_copy(lse_hbm, lsev, s_ld.at[1, 4]))
    for x in loads:
        x.start()

    def peer(i):
        return lax.rem(chip + CH + jnp.where(chip < CH // 2, i, -i), CH)

    def dev(h):
        return {'cp': h * 2 + core}

    def rcopy(src, dst, ss, rs, to):
        return pltpu.make_async_remote_copy(src_ref=src, dst_ref=dst, send_sem=ss, recv_sem=rs,
                                            device_id=to, device_id_type=MESH)

    def gather(c):
        r0 = pl.multiple_of(c * KB, KB)
        for t in range(4):
            tmp[t] = xin[t, pl.ds(r0, KB), :].astype(F32)
            for h in range(CH):
                stage[c, h, t] = tmp[t, pl.ds(h, R, stride=CH), :].astype(BF16)
        buf[c, core, chip] = stage[c, chip]

    def gather_o(c):
        tmp[4] = xin[4, pl.ds(pl.multiple_of(c * KB, KB), KB), :].astype(F32)
        for h in range(CH):
            ostage[c, h] = tmp[4, pl.ds(h, R, stride=CH), :].astype(BF16)

    def send_one(c, h):
        rcopy(stage.at[c, h], buf.at[c, core, chip], s_in.at[c], r_in.at[c], dev(h)).start()

    def send(c):
        for i in range(CH - 1, 0, -1):
            send_one(c, peer(i))

    z = chip // 2
    inner = z * (3 - z) // 2

    def far(h):
        return (h // 2 - z) * (h // 2 - z)

    def send_at(c, dist):
        for i in range(CH - 1, 0, -1):
            h = peer(i)

            @pl.when(far(h) <= 1 if dist == 1 else far(h) == dist * dist)
            def _():
                send_one(c, h)

    def tell(sem, zz):
        pl.semaphore_signal(sem, inc=1, device_id=dev(zz * 2 + chip % 2), device_id_type=MESH)

    def loop(lo, hi, f):
        lax.fori_loop(lo, hi, lambda x, _: (f(x), 0)[1], 0)

    barrier = pltpu.get_barrier_semaphore()
    pl.semaphore_signal(barrier, inc=1, device_id=sib, device_id_type=MESH)
    for i in range(CH - 1, 0, -1):
        h = peer(i)

        @pl.when(far(h) <= 1)
        def _():
            pl.semaphore_signal(barrier, inc=1, device_id=dev(h), device_id_type=MESH)
    for x in loads[:4]:
        x.wait()
    gather(C - 1)
    pl.semaphore_wait(barrier, 4 + 2 * inner)

    @pl.when(inner == 1)
    def _():
        tell(two, 3 - z)
        tell(two, 3 * (z - 1))
    send_at(C - 1, 1)
    pl.semaphore_wait(two, 1)

    @pl.when(inner == 1)
    def _():
        tell(three, 3 * (z - 1))
    send_at(C - 1, 2)

    @pl.when(inner == 0)
    def _():
        pl.semaphore_wait(three, 1)
    send_at(C - 1, 3)
    for x in loads[4:]:
        x.wait()
    gather(C - 2)
    gather(C - 3)
    send(C - 2)
    gather(C - 4)
    send(C - 3)
    loop(0, C - 4, lambda n: gather(C - 5 - n))
    send(C - 4)
    loop(0, C, gather_o)

    ones = jnp.ones((8, D), BF16)
    for h in range(CH):
        x = (stage[:, h, 3].astype(F32) * (ostage[:, h].astype(F32) * 0.5)).reshape(C * R, D)
        hi = x.astype(BF16)
        lo = (x - hi.astype(F32)).astype(BF16)
        e = (lax.dot_general(ones, hi, NT, preferred_element_type=F32)
             + lax.dot_general(ones, lo, NT, preferred_element_type=F32))
        statloc[h, :, :C * R] = lsev[h:h + 1, :]
        statloc[h, :, C * R:] = e[0:1, :] * 2.0
    statbuf[core, chip] = statloc[chip]
    for i in range(CH - 1, 0, -1):
        h = peer(i)
        rcopy(statloc.at[h], statbuf.at[core, chip], s_st.at[0], r_st.at[0], dev(h)).start()
    loop(0, C - 4, lambda n: send(C - 5 - n))

    def arrive(c):
        rcopy(buf.at[c, core, pl.ds(0, CH - 1)], buf.at[c, core, pl.ds(0, CH - 1)],
              s_in.at[c], r_in.at[c], sib).wait_recv()
        rcopy(buf.at[c, core, :, pl.ds(2, 2)], buf.at[c, core, :, pl.ds(2, 2)],
              s_fw.at[c], r_fw.at[c], sib).start()

    def forwarded(c):
        return rcopy(buf.at[c, 1 - core, :, pl.ds(2, 2)], buf.at[c, 1 - core, :, pl.ds(2, 2)],
                     s_fw.at[c], r_fw.at[c], sib)

    arrive(C - 1)
    rcopy(statbuf.at[core, pl.ds(0, CH - 1)], statbuf.at[core, pl.ds(0, CH - 1)],
          s_st.at[0], r_st.at[0], sib).wait_recv()
    fst = rcopy(statbuf.at[core], statbuf.at[core], s_st.at[1], r_st.at[1], sib)
    fst.start()
    rcopy(statbuf.at[1 - core], statbuf.at[1 - core], s_st.at[1], r_st.at[1], sib).wait_recv()
    quarter = lax.broadcasted_iota(jnp.int32, (1, 128), 1) // R
    for st in range(2):
        mul = LOG2E if st == 0 else 1.0
        for t in range(4):
            for g in range(4):
                src = [statbuf[g // 2, (g % 2) * 4 + m, :, st * 512 + t * 128:st * 512 + t * 128 + 128] * mul
                       for m in range(4)]
                for r in range(4):
                    acc = jnp.zeros((1, 128), F32)
                    for m in range(4):
                        sh = ((m - r) % 4) * R
                        x = pltpu.roll(src[m], sh, 1) if sh else src[m]
                        acc = jnp.where(quarter == m, x, acc)
                    rows[4 * t + r, st:st + 1, g * 128:(g + 1) * 128] = acc

    def diag_mask():
        ki = lax.broadcasted_iota(jnp.int32, (KB, QB), 0)
        qi = lax.broadcasted_iota(jnp.int32, (KB, QB), 1)
        kpos = (ki % R) * 16 + (ki // R) * 2 + core
        qpos = (qi % R) * 16 + ((qi // R) % CH) * 2 + qi // KB
        return kpos <= qpos

    def clear():
        dk_acc[...] = jnp.zeros_like(dk_acc)
        dv_acc[...] = jnp.zeros_like(dv_acc)

    def tile(c, b, diag):
        kk = buf[c, core, :, 0].reshape(KB, D)
        vv = buf[c, core, :, 1].reshape(KB, D)
        qq = buf[b, :, :, 2].reshape(QB, D)
        dd = buf[b, :, :, 3].reshape(QB, D)
        s = lax.dot_general(kk, qq, NT, preferred_element_type=F32)
        p = jnp.exp2(s * (SCALE * LOG2E) - rows[b, 0:1, :])
        if diag:
            p = jnp.where(diag_mask(), p, 0.0)
        dp = lax.dot_general(vv, dd, NT, preferred_element_type=F32)
        dv_acc[...] += jnp.dot(p.astype(BF16), dd, preferred_element_type=F32)
        ds = (p * (dp - rows[b, 1:2, :])).astype(BF16)
        dk_acc[...] += jnp.dot(ds, qq, preferred_element_type=F32)
        dqt = lax.dot_general(kk, ds, TN, preferred_element_type=F32)
        for y in range(2):
            part = dqt[:, y * KB:(y + 1) * KB]
            if diag:
                dq[b, y] = part
            else:
                dq[b, y] += part

    def send_kv(g):
        for i in range(CH - 1, 0, -1):
            h = peer(i)
            rcopy(kvs.at[g, h], rkv.at[g, chip], s_kv.at[g], r_kv.at[g], dev(h)).start()

    def make_kv(c):
        g = c // GK
        x = c % GK
        kvs[g, :, x, 0] = (dk_acc[...] * SCALE).astype(BF16).reshape(CH, R, D)
        kvs[g, :, x, 1] = dv_acc[...].astype(BF16).reshape(CH, R, D)
        rkv[g, chip, x] = kvs[g, chip, x]

    def step(n):
        c = C - 1 - n
        forwarded(c).wait_recv()
        clear()
        whole = n // U
        loop(0, whole, lambda u: [tile(c, c + 1 + U * u + x, False) for x in range(U)])
        loop(c + 1 + whole * U, C, lambda b: tile(c, b, False))
        arrive(c - 1)
        tile(c, c, True)
        make_kv(c)

        @pl.when(c % GK == 0)
        def _():
            send_kv(c // GK)

    loop(0, C - 1, step)

    def swap(b):
        rcopy(dq.at[b, 1 - core], dqin.at[b], s_x.at[b], r_x.at[b], sib).start()

    def give_q(b):
        rcopy(dq.at[b, core], dqin.at[b], s_x.at[b], r_x.at[b], sib).wait_recv()
        g = b // GQ
        x = b % GQ
        dqs[g, :, x] = ((dq[b, core] + dqin[b]) * SCALE).T.astype(BF16).reshape(CH, R, D)
        rq[g, chip, x] = dqs[g, chip, x]

    def send_q(g):
        for i in range(CH - 1, 0, -1):
            h = peer(i)
            rcopy(dqs.at[g, h], rq.at[g, chip], s_q.at[g], r_q.at[g], dev(h)).start()

    forwarded(0).wait_recv()
    clear()
    tile(0, 0, True)
    tile(0, 1, False)
    swap(0)
    swap(1)

    def last(u):
        tile(0, 2 * u, False)
        tile(0, 2 * u + 1, False)
        swap(2 * u)
        swap(2 * u + 1)

        @pl.when(u >= 2)
        def _():
            give_q(2 * u - 4)
            give_q(2 * u - 3)

        @pl.when((u >= 2) & ((2 * u - 2) % GQ == 0))
        def _():
            send_q((2 * u - 2) // GQ - 1)

    loop(1, C // 2, last)
    make_kv(0)
    loop(C - 4, C, give_q)
    loop((C - 4) // GQ, C // GQ, send_q)
    send_kv(0)

    def all_kv(g):
        return rcopy(kvs.at[g, pl.ds(0, CH - 1)], rkv.at[g, pl.ds(0, CH - 1)], s_kv.at[g], r_kv.at[g], sib)

    def all_q(g):
        return rcopy(dqs.at[g, pl.ds(0, CH - 1)], rq.at[g, pl.ds(0, CH - 1)], s_q.at[g], r_q.at[g], sib)

    def put_kv(n):
        g = C // GK - 1 - n
        all_kv(g).wait_recv()
        for x in range(GK):
            for t, ref in enumerate((dk_out, dv_out)):
                for h in range(CH):
                    tmp[t, pl.ds(h, R, stride=CH), :] = rkv[g, h, x, t].astype(F32)
                ref[pl.ds(pl.multiple_of((g * GK + x) * KB, KB), KB), :] = tmp[t].astype(BF16)

    loop(0, C // GK - 1, put_kv)

    def put_q(g):
        all_q(g).wait_recv()
        for x in range(GQ):
            for h in range(CH):
                tmp[x, pl.ds(h, R, stride=CH), :] = rq[g, h, x].astype(F32)
            dq_out[pl.ds(pl.multiple_of((g * GQ + x) * KB, KB), KB), :] = tmp[x].astype(BF16)

    def drain(c):
        rcopy(stage.at[c, pl.ds(0, CH - 1)], buf.at[c, core, pl.ds(0, CH - 1)], s_in.at[c], r_in.at[c], sib).wait_send()
        forwarded(c).wait_send()
        rcopy(dq.at[c, core], dqin.at[c], s_x.at[c], r_x.at[c], sib).wait_send()

    rcopy(statbuf.at[core, pl.ds(0, CH - 1)], statbuf.at[core, pl.ds(0, CH - 1)],
          s_st.at[0], r_st.at[0], sib).wait_send()
    fst.wait_send()
    loop(0, C, drain)
    loop(0, C // GQ, put_q)
    put_kv(C // GK - 1)
    loop(0, C // GK, lambda g: all_kv(g).wait_send())
    loop(0, C // GQ, lambda g: all_q(g).wait_send())


def _write(dq_ref, dk_ref, dv_ref, dq_hbm, dk_hbm, dv_hbm, sem):
    copies = [pltpu.make_async_copy(a, b, sem.at[i])
              for i, (a, b) in enumerate(((dq_ref, dq_hbm), (dk_ref, dk_hbm), (dv_ref, dv_hbm)))]
    for x in copies:
        x.start()
    for x in copies:
        x.wait()


def solution(mesh):
    rows = P(('data', 'cp'))
    cols = P(None, ('data', 'cp'))

    def local(q, k, v, o, dout, lse):
        c, h, d = q.shape
        flat = lambda x: x.reshape(c * h, d)
        vm = pl.BlockSpec(memory_space=pltpu.VMEM)
        hbm = pl.BlockSpec(memory_space=pltpu.HBM)
        sem = pltpu.SemaphoreType.DMA
        outs = pl.pallas_call(
            _kernel,
            out_shape=[pltpu.VMEM((c * h, d), BF16)] * 3,
            in_specs=[hbm] * 6,
            out_specs=[vm] * 3,
            scratch_shapes=[
                pltpu.VMEM((5, c * h, d), BF16),
                pltpu.VMEM((h, c), F32),
                pltpu.VMEM((C, CH, 4, R, D), BF16),
                pltpu.VMEM((C, CH, R, D), BF16),
                pltpu.VMEM((CH, 1, 2 * c), F32),
                pltpu.VMEM((C, 2, CH, 4, R, D), BF16),
                pltpu.VMEM((2, CH, 1, 2 * c), F32),
                pltpu.VMEM((C, 8, QB), F32),
                pltpu.VMEM((C, 2, D, KB), F32),
                pltpu.VMEM((C, D, KB), F32),
                pltpu.VMEM((C // GQ, CH, GQ, R, D), BF16),
                pltpu.VMEM((C // GK, CH, GK, 2, R, D), BF16),
                pltpu.VMEM((C // GK, CH, GK, 2, R, D), BF16),
                pltpu.VMEM((C // GQ, CH, GQ, R, D), BF16),
                pltpu.VMEM((5, KB, D), F32),
                pltpu.VMEM((KB, D), F32),
                pltpu.VMEM((KB, D), F32),
            ] + [sem((C,))] * 10 + [sem((2,))] * 2 + [sem((2, 5))] + [pltpu.SemaphoreType.REGULAR] * 2,
            compiler_params=pltpu.CompilerParams(collective_id=0, has_side_effects=True,
                                                 vmem_limit_bytes=40 * 2 ** 20),
        )(*[pltpu.with_memory_space_constraint(x, pltpu.HBM) for x in (flat(k), flat(v), flat(q), flat(dout), flat(o), lse)])
        outs = pl.pallas_call(
            _write,
            out_shape=[jax.ShapeDtypeStruct((c * h, d), BF16)] * 3,
            in_specs=[vm] * 3,
            out_specs=[hbm] * 3,
            scratch_shapes=[sem((3,))],
            compiler_params=pltpu.CompilerParams(vmem_limit_bytes=2 ** 20),
        )(*[pltpu.with_memory_space_constraint(x, pltpu.VMEM) for x in outs])
        return tuple(x.reshape(c, h, d) for x in outs)

    return jax.shard_map(local, mesh=mesh, in_specs=(rows, rows, rows, rows, rows, cols),
                         out_specs=(rows, rows, rows), check_vma=False)
```

```python
import functools
import math

import jax
import jax.numpy as jnp
from jax import lax
from jax.experimental import pallas as pl
from jax.experimental.pallas import tpu as pltpu
from jax.sharding import PartitionSpec as P

MESH = pl.DeviceIdType.MESH
F32 = jnp.float32
BF16 = jnp.bfloat16

CH = 8
R = 32
C = 16
KB = CH * R
QB = 2 * KB
D = 128
NT = (((1,), (1,)), ((), ()))
TN = (((0,), (0,)), ((), ()))
LOG2E = math.log2(math.e)
U = 4
GK = 4
GQ = 4
SCALE = D ** -0.5


def _kernel(k_hbm, v_hbm, q_hbm, do_hbm, o_hbm, lse_hbm, dq_out, dk_out, dv_out,
            xin, lsev, stage, ostage, statloc, buf, statbuf, rows, dq, dqin, dqs, kvs, rkv, rq, tmp, dk_acc, dv_acc,
            s_in, r_in, s_fw, r_fw, s_kv, r_kv, s_x, r_x, s_q, r_q, s_st, r_st, s_ld, two, three):
    cp = lax.axis_index('cp')
    chip = cp // 2
    core = cp % 2
    sib = {'cp': chip * 2 + 1 - core}

    def peer(i):
        return lax.rem(chip + CH + jnp.where(chip < CH // 2, i, -i), CH)

    def dev(h):
        return {'cp': h * 2 + core}

    z = chip // 2
    inner = z * (3 - z) // 2

    def far(h):
        return (h // 2 - z) * (h // 2 - z)

    hbm = (k_hbm, v_hbm, q_hbm, do_hbm, o_hbm)
    lead = (C - 1) * KB
    loads = []
    for t in range(4):
        loads.append(pltpu.make_async_copy(hbm[t].at[pl.ds(lead, KB)], xin.at[t, pl.ds(lead, KB)], s_ld.at[0, t]))
    for t in range(4):
        loads.append(pltpu.make_async_copy(hbm[t].at[pl.ds(0, lead)], xin.at[t, pl.ds(0, lead)], s_ld.at[1, t]))
    loads.append(pltpu.make_async_copy(o_hbm, xin.at[4], s_ld.at[0, 4]))
    loads.append(pltpu.make_async_copy(lse_hbm, lsev, s_ld.at[1, 4]))
    for x in loads[:4]:
        x.start()
    barrier = pltpu.get_barrier_semaphore()
    pl.semaphore_signal(barrier, inc=1, device_id=sib, device_id_type=MESH)
    for i in range(CH - 1, 0, -1):
        h = peer(i)

        @pl.when(far(h) <= 1)
        def _():
            pl.semaphore_signal(barrier, inc=1, device_id=dev(h), device_id_type=MESH)
    for x in loads[4:]:
        x.start()


    def rcopy(src, dst, ss, rs, to):
        return pltpu.make_async_remote_copy(src_ref=src, dst_ref=dst, send_sem=ss, recv_sem=rs,
                                            device_id=to, device_id_type=MESH)

    def gather(c):
        r0 = pl.multiple_of(c * KB, KB)
        for t in range(4):
            tmp[t] = xin[t, pl.ds(r0, KB), :].astype(F32)
            for h in range(CH):
                stage[c, h, t] = tmp[t, pl.ds(h, R, stride=CH), :].astype(BF16)
        buf[c, core, chip] = stage[c, chip]

    def gather_o(c):
        tmp[4] = xin[4, pl.ds(pl.multiple_of(c * KB, KB), KB), :].astype(F32)
        for h in range(CH):
            ostage[c, h] = tmp[4, pl.ds(h, R, stride=CH), :].astype(BF16)

    def send_one(c, h):
        rcopy(stage.at[c, h], buf.at[c, core, chip], s_in.at[c], r_in.at[c], dev(h)).start()

    def send(c):
        for i in range(CH - 1, 0, -1):
            send_one(c, peer(i))

    def send_at(c, dist):
        for i in range(CH - 1, 0, -1):
            h = peer(i)

            @pl.when(far(h) <= 1 if dist == 1 else far(h) == dist * dist)
            def _():
                send_one(c, h)

    def tell(sem, zz):
        pl.semaphore_signal(sem, inc=1, device_id=dev(zz * 2 + chip % 2), device_id_type=MESH)

    def loop(lo, hi, f):
        lax.fori_loop(lo, hi, lambda x, _: (f(x), 0)[1], 0)

    for x in loads[:4]:
        x.wait()
    gather(C - 1)
    pl.semaphore_wait(barrier, 4 + 2 * inner)

    @pl.when(inner == 1)
    def _():
        tell(two, 3 - z)
        tell(two, 3 * (z - 1))
    send_at(C - 1, 1)
    pl.semaphore_wait(two, 1)

    @pl.when(inner == 1)
    def _():
        tell(three, 3 * (z - 1))
    send_at(C - 1, 2)

    @pl.when(inner == 0)
    def _():
        pl.semaphore_wait(three, 1)
    send_at(C - 1, 3)
    for x in loads[4:]:
        x.wait()
    gather(C - 2)
    gather(C - 3)
    send(C - 2)
    gather(C - 4)
    send(C - 3)
    loop(0, C - 4, lambda n: gather(C - 5 - n))
    send(C - 4)
    loop(0, C, gather_o)

    ones = jnp.ones((8, D), BF16)
    for h in range(CH):
        x = (stage[:, h, 3].astype(F32) * (ostage[:, h].astype(F32) * 0.5)).reshape(C * R, D)
        hi = x.astype(BF16)
        lo = (x - hi.astype(F32)).astype(BF16)
        e = (lax.dot_general(ones, hi, NT, preferred_element_type=F32)
             + lax.dot_general(ones, lo, NT, preferred_element_type=F32))
        statloc[h, :, :C * R] = lsev[h:h + 1, :]
        statloc[h, :, C * R:] = e[0:1, :] * 2.0
    statbuf[core, chip] = statloc[chip]
    for i in range(CH - 1, 0, -1):
        h = peer(i)
        rcopy(statloc.at[h], statbuf.at[core, chip], s_st.at[0], r_st.at[0], dev(h)).start()
    loop(0, C - 4, lambda n: send(C - 5 - n))

    def arrive(c):
        rcopy(buf.at[c, core, pl.ds(0, CH - 1)], buf.at[c, core, pl.ds(0, CH - 1)],
              s_in.at[c], r_in.at[c], sib).wait_recv()
        rcopy(buf.at[c, core, :, pl.ds(2, 2)], buf.at[c, core, :, pl.ds(2, 2)],
              s_fw.at[c], r_fw.at[c], sib).start()

    def forwarded(c):
        return rcopy(buf.at[c, 1 - core, :, pl.ds(2, 2)], buf.at[c, 1 - core, :, pl.ds(2, 2)],
                     s_fw.at[c], r_fw.at[c], sib)

    arrive(C - 1)
    rcopy(statbuf.at[core, pl.ds(0, CH - 1)], statbuf.at[core, pl.ds(0, CH - 1)],
          s_st.at[0], r_st.at[0], sib).wait_recv()
    fst = rcopy(statbuf.at[core], statbuf.at[core], s_st.at[1], r_st.at[1], sib)
    fst.start()
    rcopy(statbuf.at[1 - core], statbuf.at[1 - core], s_st.at[1], r_st.at[1], sib).wait_recv()
    quarter = lax.broadcasted_iota(jnp.int32, (1, 128), 1) // R
    for st in range(2):
        mul = LOG2E if st == 0 else 1.0
        for t in range(4):
            for g in range(4):
                src = [statbuf[g // 2, (g % 2) * 4 + m, :, st * 512 + t * 128:st * 512 + t * 128 + 128] * mul
                       for m in range(4)]
                for r in range(4):
                    acc = jnp.zeros((1, 128), F32)
                    for m in range(4):
                        sh = ((m - r) % 4) * R
                        x = pltpu.roll(src[m], sh, 1) if sh else src[m]
                        acc = jnp.where(quarter == m, x, acc)
                    rows[4 * t + r, st:st + 1, g * 128:(g + 1) * 128] = acc

    def diag_mask():
        ki = lax.broadcasted_iota(jnp.int32, (KB, QB), 0)
        qi = lax.broadcasted_iota(jnp.int32, (KB, QB), 1)
        kpos = (ki % R) * 16 + (ki // R) * 2 + core
        qpos = (qi % R) * 16 + ((qi // R) % CH) * 2 + qi // KB
        return kpos <= qpos

    def clear():
        dk_acc[...] = jnp.zeros_like(dk_acc)
        dv_acc[...] = jnp.zeros_like(dv_acc)

    def tile(c, b, diag):
        kk = buf[c, core, :, 0].reshape(KB, D)
        vv = buf[c, core, :, 1].reshape(KB, D)
        qq = buf[b, :, :, 2].reshape(QB, D)
        dd = buf[b, :, :, 3].reshape(QB, D)
        s = lax.dot_general(kk, qq, NT, preferred_element_type=F32)
        p = jnp.exp2(s * (SCALE * LOG2E) - rows[b, 0:1, :])
        if diag:
            p = jnp.where(diag_mask(), p, 0.0)
        dp = lax.dot_general(vv, dd, NT, preferred_element_type=F32)
        dv_acc[...] += jnp.dot(p.astype(BF16), dd, preferred_element_type=F32)
        ds = (p * (dp - rows[b, 1:2, :])).astype(BF16)
        dk_acc[...] += jnp.dot(ds, qq, preferred_element_type=F32)
        dqt = lax.dot_general(kk, ds, TN, preferred_element_type=F32)
        for y in range(2):
            part = dqt[:, y * KB:(y + 1) * KB]
            if diag:
                dq[b, y] = part
            else:
                dq[b, y] += part

    def send_kv(g):
        for i in range(CH - 1, 0, -1):
            h = peer(i)
            rcopy(kvs.at[g, h], rkv.at[g, chip], s_kv.at[g], r_kv.at[g], dev(h)).start()

    def make_kv(c):
        g = c // GK
        x = c % GK
        kvs[g, :, x, 0] = (dk_acc[...] * SCALE).astype(BF16).reshape(CH, R, D)
        kvs[g, :, x, 1] = dv_acc[...].astype(BF16).reshape(CH, R, D)
        rkv[g, chip, x] = kvs[g, chip, x]

    def step(n):
        c = C - 1 - n
        forwarded(c).wait_recv()
        clear()
        whole = n // U
        loop(0, whole, lambda u: [tile(c, c + 1 + U * u + x, False) for x in range(U)])
        arrive(c - 1)
        loop(c + 1 + whole * U, C, lambda b: tile(c, b, False))
        tile(c, c, True)
        make_kv(c)

        @pl.when(c % GK == 0)
        def _():
            send_kv(c // GK)

    loop(0, C - 1, step)

    def swap(b):
        rcopy(dq.at[b, 1 - core], dqin.at[b], s_x.at[b], r_x.at[b], sib).start()

    def give_q(b):
        rcopy(dq.at[b, core], dqin.at[b], s_x.at[b], r_x.at[b], sib).wait_recv()
        g = b // GQ
        x = b % GQ
        dqs[g, :, x] = ((dq[b, core] + dqin[b]) * SCALE).T.astype(BF16).reshape(CH, R, D)
        rq[g, chip, x] = dqs[g, chip, x]

    def send_q(g):
        for i in range(CH - 1, 0, -1):
            h = peer(i)
            rcopy(dqs.at[g, h], rq.at[g, chip], s_q.at[g], r_q.at[g], dev(h)).start()

    forwarded(0).wait_recv()
    clear()
    tile(0, 0, True)
    tile(0, 1, False)
    swap(0)
    swap(1)

    def last(u):
        tile(0, 2 * u, False)
        tile(0, 2 * u + 1, False)
        swap(2 * u)
        swap(2 * u + 1)

        @pl.when(u >= 2)
        def _():
            give_q(2 * u - 4)
            give_q(2 * u - 3)

        @pl.when((u >= 2) & ((2 * u - 2) % GQ == 0))
        def _():
            send_q((2 * u - 2) // GQ - 1)

    loop(1, C // 2, last)
    make_kv(0)
    loop(C - 4, C, give_q)
    loop((C - 4) // GQ, C // GQ, send_q)
    send_kv(0)

    def all_kv(g):
        return rcopy(kvs.at[g, pl.ds(0, CH - 1)], rkv.at[g, pl.ds(0, CH - 1)], s_kv.at[g], r_kv.at[g], sib)

    def all_q(g):
        return rcopy(dqs.at[g, pl.ds(0, CH - 1)], rq.at[g, pl.ds(0, CH - 1)], s_q.at[g], r_q.at[g], sib)

    def put_kv(n):
        g = C // GK - 1 - n
        all_kv(g).wait_recv()
        for x in range(GK):
            for t, ref in enumerate((dk_out, dv_out)):
                for h in range(CH):
                    tmp[t, pl.ds(h, R, stride=CH), :] = rkv[g, h, x, t].astype(F32)
                ref[pl.ds(pl.multiple_of((g * GK + x) * KB, KB), KB), :] = tmp[t].astype(BF16)

    loop(0, C // GK - 1, put_kv)

    def put_q(g):
        all_q(g).wait_recv()
        for x in range(GQ):
            for h in range(CH):
                tmp[x, pl.ds(h, R, stride=CH), :] = rq[g, h, x].astype(F32)
            dq_out[pl.ds(pl.multiple_of((g * GQ + x) * KB, KB), KB), :] = tmp[x].astype(BF16)

    def drain(c):
        rcopy(stage.at[c, pl.ds(0, CH - 1)], buf.at[c, core, pl.ds(0, CH - 1)], s_in.at[c], r_in.at[c], sib).wait_send()
        forwarded(c).wait_send()
        rcopy(dq.at[c, core], dqin.at[c], s_x.at[c], r_x.at[c], sib).wait_send()

    rcopy(statbuf.at[core, pl.ds(0, CH - 1)], statbuf.at[core, pl.ds(0, CH - 1)],
          s_st.at[0], r_st.at[0], sib).wait_send()
    fst.wait_send()
    loop(0, C, drain)
    loop(0, C // GQ, put_q)
    put_kv(C // GK - 1)
    loop(0, C // GK, lambda g: all_kv(g).wait_send())
    loop(0, C // GQ, lambda g: all_q(g).wait_send())


def _write(dq_ref, dk_ref, dv_ref, dq_hbm, dk_hbm, dv_hbm, sem):
    copies = [pltpu.make_async_copy(a, b, sem.at[i])
              for i, (a, b) in enumerate(((dq_ref, dq_hbm), (dk_ref, dk_hbm), (dv_ref, dv_hbm)))]
    for x in copies:
        x.start()
    for x in copies:
        x.wait()


def solution(mesh):
    rows = P(('data', 'cp'))
    cols = P(None, ('data', 'cp'))

    def local(q, k, v, o, dout, lse):
        c, h, d = q.shape
        flat = lambda x: x.reshape(c * h, d)
        vm = pl.BlockSpec(memory_space=pltpu.VMEM)
        hbm = pl.BlockSpec(memory_space=pltpu.HBM)
        sem = pltpu.SemaphoreType.DMA
        outs = pl.pallas_call(
            _kernel,
            out_shape=[pltpu.VMEM((c * h, d), BF16)] * 3,
            in_specs=[hbm] * 6,
            out_specs=[vm] * 3,
            scratch_shapes=[
                pltpu.VMEM((5, c * h, d), BF16),
                pltpu.VMEM((h, c), F32),
                pltpu.VMEM((C, CH, 4, R, D), BF16),
                pltpu.VMEM((C, CH, R, D), BF16),
                pltpu.VMEM((CH, 1, 2 * c), F32),
                pltpu.VMEM((C, 2, CH, 4, R, D), BF16),
                pltpu.VMEM((2, CH, 1, 2 * c), F32),
                pltpu.VMEM((C, 8, QB), F32),
                pltpu.VMEM((C, 2, D, KB), F32),
                pltpu.VMEM((C, D, KB), F32),
                pltpu.VMEM((C // GQ, CH, GQ, R, D), BF16),
                pltpu.VMEM((C // GK, CH, GK, 2, R, D), BF16),
                pltpu.VMEM((C // GK, CH, GK, 2, R, D), BF16),
                pltpu.VMEM((C // GQ, CH, GQ, R, D), BF16),
                pltpu.VMEM((5, KB, D), F32),
                pltpu.VMEM((KB, D), F32),
                pltpu.VMEM((KB, D), F32),
            ] + [sem((C,))] * 10 + [sem((2,))] * 2 + [sem((2, 5))] + [pltpu.SemaphoreType.REGULAR] * 2,
            compiler_params=pltpu.CompilerParams(collective_id=0, has_side_effects=True,
                                                 vmem_limit_bytes=40 * 2 ** 20),
        )(*[pltpu.with_memory_space_constraint(x, pltpu.HBM) for x in (flat(k), flat(v), flat(q), flat(dout), flat(o), lse)])
        outs = pl.pallas_call(
            _write,
            out_shape=[jax.ShapeDtypeStruct((c * h, d), BF16)] * 3,
            in_specs=[vm] * 3,
            out_specs=[hbm] * 3,
            scratch_shapes=[sem((3,))],
            compiler_params=pltpu.CompilerParams(vmem_limit_bytes=2 ** 20),
        )(*[pltpu.with_memory_space_constraint(x, pltpu.VMEM) for x in outs])
        return tuple(x.reshape(c, h, d) for x in outs)

    return jax.shard_map(local, mesh=mesh, in_specs=(rows, rows, rows, rows, rows, cols),
                         out_specs=(rows, rows, rows), check_vma=False)
```
